32 devices in a mesh: gx: 4 (over x, core), gy: 4 (over z), gz: 2 (over y).
Axes of the slice: x: 2, y: 2, z: 4, core: 2. Of those that a mesh axis runs over, the one named last changes fastest.
Arguments:
- grad_bucket: bfloat16 [32, 1, 3584, 1024], P(('gx', 'gy', 'gz')), may hold values from -72000 to 72000
- parameters: bfloat16 [1, 3584, 1024], P(None, ('gx', 'gy', 'gz')), may hold values from -4 to 4
- row_state: float32 [1, 3584], P(None, ('gx', 'gy', 'gz')), may hold values from 0.01 to 10
- column_state: float32 [1, 1024], replicated, may hold values from 0.01 to 10
Outputs:
- new_parameters: bfloat16 [1, 3584, 1024], P(None, ('gx', 'gy', 'gz'))
- row_next: float32 [1, 3584], P(None, ('gx', 'gy', 'gz'))
- column_next: float32 [1, 1024], replicated
- first_layer: bfloat16 [3584, 1024], replicated
The draws below stay inside these ranges and needn't reach their ends.
All inputs are finite; a program needn't handle non-finite values.
Results may differ from the reference program's by a relative error of at most 0.011.
Values may be sent and summed in bfloat16 or wider, within the bound.
A program may use at most 128 MiB of HBM per device.

```python
import math
import jax
import jax.numpy as jnp
from jax import lax

D = 3584
LAYERS = 1
KW = 1024
DEVICES = 32


def draw_grad_bucket(key, part):
    row_key = jax.random.fold_in(key, 11)
    column_key = jax.random.fold_in(key, 12)
    owner_key = jax.random.fold_in(key, 13)
    row_index = jnp.arange(D, dtype=jnp.int32)
    rising = jnp.exp(math.log(3.0) * row_index.astype(jnp.float32) / (D - 1))
    row_scale = rising[None, :] * jnp.exp(math.log(10.0) * jax.random.uniform(row_key, (LAYERS, D)))
    column_scale = jnp.exp(math.log(10.0) * jax.random.uniform(column_key, (LAYERS, KW)))
    owners = jax.random.permutation(owner_key, DEVICES).astype(jnp.int32)
    row_owner = row_index // (D // DEVICES)

    def one_device(device):
        device_key = jax.random.fold_in(key, 1000 + device)
        noise_part = jnp.clip(jax.random.normal(device_key, (LAYERS, D, KW)), -6.0, 6.0)
        spiked = jnp.where(row_owner == owners[device], 24.0, 1.0)
        values = noise_part * row_scale[:, :, None] * column_scale[:, None, :] * spiked[None, :, None]
        return values.astype(jnp.bfloat16)
    return lax.map(one_device, jnp.arange(DEVICES, dtype=jnp.int32))


def steps_of(rng, dims, pieces, low, high):
    loudness, own = 1.0, jax.random.fold_in(rng, 6)
    for axis_at, shards_of in pieces:
        steps = jnp.exp(jax.random.uniform(jax.random.fold_in(own, axis_at), (shards_of,), jnp.float32, low / len(pieces), high / len(pieces)))
        loudness = loudness * jnp.repeat(steps, dims[axis_at] // shards_of).reshape([-1 if axis == axis_at else 1 for axis in range(len(dims))])
    return loudness


def normal_values(stream_key, extent, scale, most, shards=(), kind=jnp.bfloat16):
    array = scale * jax.random.normal(stream_key, extent, jnp.float32)
    if shards:
        array = array * steps_of(stream_key, extent, shards, -0.22, 0.18)
    return jnp.clip(array, -most, most).astype(kind)


def setup_inputs(seed: int = 0) -> dict:
    key_of = jax.random.split(jax.random.key(seed), 5)
    grad_bucket = draw_grad_bucket(jax.random.fold_in(key_of[4], 71), 0)
    parameters = normal_values(key_of[1], (LAYERS, D, KW), 1.0, 4.0, ((1, 32),))
    row_state = jnp.clip(jnp.exp(math.log(10.0) - 6.9077553 * jax.random.uniform(key_of[2], (LAYERS, D), jnp.float32) ** steps_of(key_of[2], (LAYERS, D), ((1, 32),), -0.2, 0.2)), 0.01, 10.0)
    column_state = jnp.clip(jnp.exp(jax.random.uniform(key_of[3], (LAYERS, KW), jnp.float32, math.log(0.01), math.log(10.0))), 0.01, 10.0)
    return dict(grad_bucket=grad_bucket, parameters=parameters, row_state=row_state, column_state=column_state)


beta_two = 0.8
step_size = 0.5

def reference(grad_bucket, parameters, row_state, column_state):

    def accumulate(running, device_grad):
        return (running + device_grad.astype(jnp.float32), None)
    summed, unused = lax.scan(accumulate, jnp.zeros((LAYERS, D, KW), jnp.float32), grad_bucket)
    norm_square = jnp.sum(summed * summed)
    clip_level = 0.5 * math.sqrt(LAYERS * D * KW)
    factor = jnp.minimum(jnp.float32(1.0), clip_level / jnp.sqrt(norm_square + 1e-06))
    clipped = factor * summed
    squares = clipped * clipped
    row_next = beta_two * row_state + (1.0 - beta_two) * lax.optimization_barrier(jnp.mean(squares, axis=2))
    column_next = beta_two * column_state + (1.0 - beta_two) * lax.optimization_barrier(jnp.mean(squares, axis=1))
    row_average = lax.optimization_barrier(jnp.mean(row_next, axis=1))
    second = row_next[:, :, None] * column_next[:, None, :] / row_average[:, None, None]
    update = clipped / jnp.sqrt(second)
    new_parameters = (parameters.astype(jnp.float32) - step_size * update).astype(jnp.bfloat16)
    return (new_parameters, row_next, column_next, new_parameters[0])
```

```python
import functools
import math

import jax
import jax.numpy as jnp
from jax import lax
from jax.experimental import pallas as pl
from jax.experimental.pallas import tpu as pltpu
from jax.sharding import PartitionSpec as P

beta_two = 0.8
step_size = 0.5
AXES = ("gx", "gy", "gz")
TILE = 16


def shards(grad_bucket, parameters, row_state, column_state):
    local_grad = grad_bucket[0].astype(jnp.float32)
    layer_count, full_width, columns = local_grad.shape
    summed = lax.psum_scatter(local_grad, AXES, scatter_dimension=1, tiled=True)
    clip_level = 0.5 * math.sqrt(layer_count * full_width * columns)
    squares = summed * summed
    norm_square = lax.psum(jnp.sum(squares), AXES)
    factor = jnp.minimum(jnp.float32(1.0), clip_level / jnp.sqrt(norm_square + 1e-06))
    clipped = factor * summed
    clipped_square = clipped * clipped
    row_next = beta_two * row_state + (1.0 - beta_two) * jnp.mean(clipped_square, axis=2)
    column_part, row_total = lax.psum((jnp.sum(clipped_square, axis=1), jnp.sum(row_next, axis=1)), AXES)
    column_next = beta_two * column_state + (1.0 - beta_two) * column_part / full_width
    row_average = row_total / full_width
    second = row_next[:, :, None] * column_next[:, None, :] / row_average[:, None, None]
    update = clipped / jnp.sqrt(second)
    new_parameters = (parameters.astype(jnp.float32) - step_size * update).astype(jnp.bfloat16)
    first_layer = lax.all_gather(new_parameters[0], AXES, axis=0, tiled=True)
    return (new_parameters, row_next, column_next, first_layer)


def flip(index, mask, size):
    out, bit = 0, 1
    while bit < size:
        out = out + bit * (((index // bit) % 2 + (mask // bit) % 2) % 2)
        bit *= 2
    return out


def kernel(nx, nz, grad, params, row_state, col_state, new_ref, row_ref, col_ref, full,
           lg, cr, r1a, r1b, r2a, r2b, rz, summed, own, st, st1, tot, st2,
           lsem, cs, crv, p1as, p1ar, p1bs, p1br, p2as, p2ar, p2bs, p2br, zs, zr,
           s1s, s1r, s2s, s2r, gzs, gzr, q1as, q1ar, q1bs, q1br, q2as, q2ar, q2bs, q2br, gcs, gcr):
    gx, z, y = lax.axis_index("gx"), lax.axis_index("gy"), lax.axis_index("gz")
    x, c = gx // 2, gx % 2
    rows, columns = params.shape
    half = columns // 2
    full_width = rows * 4 * nz * 2
    core_peer = (x * 2 + 1 - c, z, y)
    x_peer = ((1 - x) * 2 + c, z, y)
    y_peer = (gx, z, 1 - y)
    lo, hi = pl.ds(0, half), pl.ds(half, half)
    tiles = rows // TILE

    def zof(t):
        return flip(z, t, nz)

    def rdma(src, dst, ssem, rsem, peer):
        return pltpu.make_async_remote_copy(
            src_ref=src, dst_ref=dst, send_sem=ssem, recv_sem=rsem,
            device_id=peer, device_id_type=pl.DeviceIdType.MESH)

    rs_order = list(range(nz - 1, -1, -1))
    if nz == 4:
        rs_order = [2, 3, 1, 0]
    loads = {t: pltpu.make_async_copy(grad.at[:, c, zof(t)], lg.at[t], lsem.at[t]) for t in rs_order}
    for t in rs_order:
        loads[t].start()

    barrier = pltpu.get_barrier_semaphore()
    plane = [((gx + a) % nx, z, (y + b) % 2) for a in range(nx) for b in range(2) if (a, b) != (0, 0)]
    line = [(gx, zof(t), y) for t in range(1, nz)]
    for peer in plane + line:
        pl.semaphore_signal(barrier, inc=1, device_id=peer, device_id_type=pl.DeviceIdType.MESH)
    pl.semaphore_wait(barrier, len(plane) + len(line))

    core = {t: rdma(grad.at[:, 1 - c, zof(t)], cr.at[t], cs.at[t], crv.at[t], core_peer) for t in rs_order}
    for t in rs_order:
        core[t].start()
    p1a = {t: rdma(lg.at[t, 1 - x, :, :, lo], r1a.at[t], p1as.at[t], p1ar.at[t], x_peer) for t in rs_order}
    p1b = {t: rdma(lg.at[t, :, 1 - y, :, hi], r1b.at[t], p1bs.at[t], p1br.at[t], y_peer) for t in rs_order}
    p2a = {t: rdma(lg.at[t, x, 1 - y, :, lo], r2a.at[t], p2as.at[t], p2ar.at[t], y_peer) for t in rs_order}
    p2b = {t: rdma(lg.at[t, 1 - x, y, :, hi], r2b.at[t], p2bs.at[t], p2br.at[t], x_peer) for t in rs_order}
    zc = {t: rdma(lg.at[t, x, y], rz.at[t], zs.at[t], zr.at[t], (gx, zof(t), y)) for t in range(1, nz)}

    def add(a, b):
        return (a.astype(jnp.float32) + b.astype(jnp.float32)).astype(jnp.bfloat16)

    def stage_core(t):
        loads[t].wait()
        core[t].wait_recv()

        @pl.loop(0, tiles)
        def _(i):
            r = pl.ds(pl.multiple_of(i * TILE, TILE), TILE)
            for a in range(2):
                for b in range(2):
                    lg[t, a, b, r, :] = add(lg[t, a, b, r, :], cr[t, a, b, r, :])
        p1a[t].start()
        p1b[t].start()

    def stage_one(t):
        p1a[t].wait_recv()
        p1b[t].wait_recv()

        @pl.loop(0, tiles)
        def _(i):
            r = pl.ds(pl.multiple_of(i * TILE, TILE), TILE)
            for b in range(2):
                lg[t, x, b, r, lo] = add(lg[t, x, b, r, lo], r1a[t, b, r, :])
                lg[t, b, y, r, hi] = add(lg[t, b, y, r, hi], r1b[t, b, r, :])
        p2a[t].start()
        p2b[t].start()

    def stage_two(t):
        p2a[t].wait_recv()
        p2b[t].wait_recv()
        if t == 0:
            return

        @pl.loop(0, tiles)
        def _(i):
            r = pl.ds(pl.multiple_of(i * TILE, TILE), TILE)
            lg[t, x, y, r, lo] = add(lg[t, x, y, r, lo], r2a[t, r, :])
            lg[t, x, y, r, hi] = add(lg[t, x, y, r, hi], r2b[t, r, :])
        zc[t].start()

    n = len(rs_order)
    stage_core(rs_order[0])
    stage_core(rs_order[1])
    for i in range(n + 1):
        if i < n:
            stage_one(rs_order[i])
        if i + 2 < n:
            stage_core(rs_order[i + 2])
        if i >= 1:
            stage_two(rs_order[i - 1])
    for t in rs_order:
        if t:
            zc[t].wait_recv()

    def final(i, carry):
        r = pl.ds(pl.multiple_of(i * TILE, TILE), TILE)
        f32 = jnp.float32
        left = lg[0, x, y, r, lo].astype(f32) + r2a[0, r, :].astype(f32)
        right = lg[0, x, y, r, hi].astype(f32) + r2b[0, r, :].astype(f32)
        for t in range(1, nz):
            left = left + rz[t, r, lo].astype(f32)
            right = right + rz[t, r, hi].astype(f32)
        summed[r, lo] = left
        summed[r, hi] = right
        left, right = left * left, right * right
        own[r, :] = jnp.sum(left, axis=1, keepdims=True) + jnp.sum(right, axis=1, keepdims=True)
        return (carry[0] + left, carry[1] + right)

    zero = jnp.zeros((TILE, half), jnp.float32)
    left, right = lax.fori_loop(0, tiles, final, (zero, zero))
    st[0:1, lo] = jnp.sum(left, axis=0, keepdims=True)
    st[0:1, hi] = jnp.sum(right, axis=0, keepdims=True)
    st[1:2, :] = jnp.broadcast_to(jnp.sum(row_state[...], axis=1, keepdims=True), (1, columns))

    me = gx * 2 + y
    sends = []
    for k, (a, b) in enumerate([(a, b) for a in range(nx) for b in range(2) if (a, b) != (0, 0)]):
        sends.append(rdma(st, st1.at[me], s1s.at[k], s1r.at[k], ((gx + a) % nx, z, (y + b) % 2)))
        sends[-1].start()
    st1[me] = st[...]
    for copy in sends:
        copy.wait_recv()
    total = st1[0]
    for k in range(1, nx * 2):
        total = total + st1[k]
    tot[...] = total
    line_sends = []
    for t in range(1, nz):
        line_sends.append(rdma(tot, st2.at[z], s2s.at[t], s2r.at[t], (gx, zof(t), y)))
        line_sends[-1].start()
    st2[z] = total
    for t in rs_order:
        core[t].wait_send()
        for copy in (p1a[t], p1b[t], p2a[t], p2b[t]):
            copy.wait_send()
        if t:
            zc[t].wait_send()
    for copy in line_sends:
        copy.wait_recv()
    total = st2[0]
    for k in range(1, nz):
        total = total + st2[k]
    column_sum = total[0:1, :]
    norm_square = jnp.sum(column_sum, axis=1, keepdims=True)
    state_sum = total[1:2, 0:1]
    clip_level = 0.5 * math.sqrt(full_width * columns)
    factor = jnp.minimum(jnp.float32(1.0), clip_level / jnp.sqrt(norm_square + 1e-06))
    square_factor = factor * factor
    column_next = beta_two * col_state[...] + (1.0 - beta_two) * (square_factor * column_sum / full_width)
    col_ref[...] = column_next
    row_average = (beta_two * state_sum + (1.0 - beta_two) * (square_factor * norm_square / columns)) / full_width
    diagonal = lax.broadcasted_iota(jnp.int32, (rows, rows), 0) == lax.broadcasted_iota(jnp.int32, (rows, rows), 1)
    state_down = jnp.sum(jnp.where(diagonal, jnp.broadcast_to(row_state[...], (rows, rows)), 0.0), axis=1, keepdims=True)
    row_next = beta_two * state_down + (1.0 - beta_two) * (square_factor * own[...] / columns)
    row_ref[...] = jnp.sum(jnp.where(diagonal, jnp.broadcast_to(row_next, (rows, rows)), 0.0), axis=0, keepdims=True)
    own[...] = (step_size * factor) / jnp.sqrt(row_next / row_average)
    col_scale = 1.0 / jnp.sqrt(column_next)

    @pl.loop(0, tiles)
    def _(i):
        r = pl.ds(pl.multiple_of(i * TILE, TILE), TILE)
        new = params[r, :].astype(jnp.float32) - (summed[r, :] * own[r, :]) * col_scale
        new = new.astype(jnp.bfloat16)
        full[x, c, z, y, r, :] = new
        new_ref[r, :] = new

    gz = {t: rdma(full.at[x, c, z, y], full.at[x, c, z, y], gzs.at[t], gzr.at[t], (gx, zof(t), y)) for t in range(1, nz)}

    def same(view, ssem, rsem, peer):
        return rdma(view, view, ssem, rsem, peer)

    q1a, q1b, q2a, q2b, gc = {}, {}, {}, {}, {}
    for t in range(nz):
        u = zof(t)
        q1a[t] = same(full.at[x, c, u, y, :, lo], q1as.at[t], q1ar.at[t], y_peer)
        q1b[t] = same(full.at[x, c, u, y, :, hi], q1bs.at[t], q1br.at[t], x_peer)
        q2a[t] = same(full.at[x, c, u, :, :, lo], q2as.at[t], q2ar.at[t], x_peer)
        q2b[t] = same(full.at[:, c, u, y, :, hi], q2bs.at[t], q2br.at[t], y_peer)
        gc[t] = same(full.at[:, c, u], gcs.at[t], gcr.at[t], core_peer)

    def gather_one(t):
        if t:
            gz[t].wait_recv()
        q1a[t].start()
        q1b[t].start()

    def gather_two(t):
        q1a[t].wait_recv()
        q1b[t].wait_recv()
        q2a[t].start()
        q2b[t].start()

    def gather_core(t):
        q2a[t].wait_recv()
        q2b[t].wait_recv()
        gc[t].start()

    q1a[0].start()
    q1b[0].start()
    for t in range(1, nz):
        gz[t].start()
    gather_two(0)
    for t in range(1, nz):
        gather_one(t)
        gather_core(t - 1)
        gather_two(t)
    gather_core(nz - 1)
    for copy in sends + line_sends:
        copy.wait_send()
    for t in range(nz):
        if t:
            gz[t].wait_send()
        for copy in (q1a[t], q1b[t], q2a[t], q2b[t]):
            copy.wait_send()
        gc[t].wait_send()
        gc[t].wait_recv()


def fused(nx, nz, grad_bucket, parameters, row_state, column_state):
    _, _, full_width, columns = grad_bucket.shape
    rows = parameters.shape[1]
    half = columns // 2
    bf16, f32 = jnp.bfloat16, jnp.float32
    vmem = pl.BlockSpec(memory_space=pltpu.VMEM)
    dma = pltpu.SemaphoreType.DMA
    new, row, col, full = pl.pallas_call(
        functools.partial(kernel, nx, nz),
        out_shape=(
            jax.ShapeDtypeStruct((rows, columns), bf16),
            jax.ShapeDtypeStruct((1, rows), f32),
            jax.ShapeDtypeStruct((1, columns), f32),
            jax.ShapeDtypeStruct((2, 2, nz, 2, rows, columns), bf16),
        ),
        in_specs=[pl.BlockSpec(memory_space=pl.ANY), vmem, vmem, vmem],
        out_specs=(vmem, vmem, vmem, vmem),
        scratch_shapes=[
            pltpu.VMEM((nz, 2, 2, rows, columns), bf16),
            pltpu.VMEM((nz, 2, 2, rows, columns), bf16),
            pltpu.VMEM((nz, 2, rows, half), bf16),
            pltpu.VMEM((nz, 2, rows, half), bf16),
            pltpu.VMEM((nz, rows, half), bf16),
            pltpu.VMEM((nz, rows, half), bf16),
            pltpu.VMEM((nz, rows, columns), bf16),
            pltpu.VMEM((rows, columns), f32),
            pltpu.VMEM((rows, 1), f32),
            pltpu.VMEM((2, columns), f32),
            pltpu.VMEM((nx * 2, 2, columns), f32),
            pltpu.VMEM((2, columns), f32),
            pltpu.VMEM((nz, 2, columns), f32),
        ] + [dma((nz,))] * 13 + [dma((nx * 2,))] * 2 + [dma((nz,))] * 14,
        compiler_params=pltpu.CompilerParams(
            collective_id=0, has_side_effects=True, vmem_limit_bytes=48 * 1024 * 1024),
    )(grad_bucket.reshape(2, 2, nz, 2, rows, columns), parameters[0], row_state, column_state)
    return (new[None], row, col, full.reshape(full_width, columns))


def solution(mesh):
    nx, nz, ny = (mesh.shape[a] for a in AXES)
    in_specs = (
        P(AXES, None, None, None),
        P(None, AXES, None),
        P(None, AXES),
        P(),
    )
    out_specs = (P(None, AXES, None), P(None, AXES), P(), P())
    fits = nx == 4 and ny == 2 and nz & (nz - 1) == 0

    def body(grad_bucket, parameters, row_state, column_state):
        if fits and grad_bucket.shape[1] == 1 and parameters.shape[1] % TILE == 0:
            return fused(nx, nz, grad_bucket, parameters, row_state, column_state)
        return shards(grad_bucket, parameters, row_state, column_state)

    return jax.shard_map(body, mesh=mesh, in_specs=in_specs, out_specs=out_specs, check_vma=False)
```

```python
import functools
import math

import jax
import jax.numpy as jnp
from jax import lax
from jax.experimental import pallas as pl
from jax.experimental.pallas import tpu as pltpu
from jax.sharding import PartitionSpec as P

beta_two = 0.8
step_size = 0.5
AXES = ("gx", "gy", "gz")
TILE = 16
VMEM_BYTES = 67043328 - 131072


def shards(grad_bucket, parameters, row_state, column_state):
    local_grad = grad_bucket[0].astype(jnp.float32)
    layer_count, full_width, columns = local_grad.shape
    summed = lax.psum_scatter(local_grad, AXES, scatter_dimension=1, tiled=True)
    clip_level = 0.5 * math.sqrt(layer_count * full_width * columns)
    squares = summed * summed
    norm_square = lax.psum(jnp.sum(squares), AXES)
    factor = jnp.minimum(jnp.float32(1.0), clip_level / jnp.sqrt(norm_square + 1e-06))
    clipped = factor * summed
    clipped_square = clipped * clipped
    row_next = beta_two * row_state + (1.0 - beta_two) * jnp.mean(clipped_square, axis=2)
    column_part, row_total = lax.psum((jnp.sum(clipped_square, axis=1), jnp.sum(row_next, axis=1)), AXES)
    column_next = beta_two * column_state + (1.0 - beta_two) * column_part / full_width
    row_average = row_total / full_width
    second = row_next[:, :, None] * column_next[:, None, :] / row_average[:, None, None]
    update = clipped / jnp.sqrt(second)
    new_parameters = (parameters.astype(jnp.float32) - step_size * update).astype(jnp.bfloat16)
    first_layer = lax.all_gather(new_parameters[0], AXES, axis=0, tiled=True)
    return (new_parameters, row_next, column_next, first_layer)


def flip(index, mask, size):
    out, bit = 0, 1
    while bit < size:
        out = out + bit * (((index // bit) % 2 + (mask // bit) % 2) % 2)
        bit *= 2
    return out


def kernel(nx, nz, grad, params_in, row_in, col_in, new_ref, row_ref, col_ref, full,
           lg, cr, r1a, r1b, r2a, r2b, rz, summed, own, st, st1, tot, st2, params, row_state, col_state,
           lsem, isem, cs, crv, fas, far, fbs, fbr, gas, gar, gbs, gbr, has, har, hbs, hbr, zs, zr,
           s1s, s1r, s2s, s2r, gzs, gzr, q1as, q1ar, q1bs, q1br, q2as, q2ar, q2bs, q2br,
           q3as, q3ar, q3bs, q3br, gcs, gcr):
    gx, z, y = lax.axis_index("gx"), lax.axis_index("gy"), lax.axis_index("gz")
    x, c = gx // 2, gx % 2
    rows, columns = params.shape
    half = columns // 2
    full_width = rows * 4 * nz * 2
    core_peer = (x * 2 + 1 - c, z, y)
    x_peer = ((1 - x) * 2 + c, z, y)
    y_peer = (gx, z, 1 - y)
    lo, hi = pl.ds(0, half), pl.ds(half, half)
    tiles = rows // TILE
    f32 = jnp.float32
    blocks = [(1 - x, 1 - y), (1 - x, y), (x, 1 - y), (x, y)]

    def zof(t):
        return flip(z, t, nz)

    def rdma(src, dst, ssem, rsem, peer):
        return pltpu.make_async_remote_copy(
            src_ref=src, dst_ref=dst, send_sem=ssem, recv_sem=rsem,
            device_id=peer, device_id_type=pl.DeviceIdType.MESH)

    rs_order = [2, 3, 1, 0] if nz == 4 else list(range(nz - 1, -1, -1))
    loads = {t: pltpu.make_async_copy(grad.at[:, c, zof(t)], lg.at[t], lsem.at[t]) for t in rs_order}
    for t in rs_order:
        loads[t].start()
    small = [pltpu.make_async_copy(src, dst, isem.at[k]) for k, (src, dst) in enumerate(
        [(params_in, params), (row_in, row_state), (col_in, col_state)])]
    for copy in small:
        copy.start()

    barrier = pltpu.get_barrier_semaphore()
    plane = [((gx + a) % nx, z, (y + b) % 2) for a in range(nx) for b in range(2) if (a, b) != (0, 0)]
    line = [(gx, zof(t), y) for t in range(1, nz)]
    for peer in line + plane:
        pl.semaphore_signal(barrier, inc=1, device_id=peer, device_id_type=pl.DeviceIdType.MESH)
    pl.semaphore_wait(barrier, len(plane) + len(line))

    core, fa, fb, ga, gb, ha, hb, zc = {}, {}, {}, {}, {}, {}, {}, {}
    for t in rs_order:
        for k, (bx, by) in enumerate(blocks):
            core[t, k] = rdma(grad.at[bx, 1 - c, zof(t), by], cr.at[t, k], cs.at[t, k], crv.at[t, k], core_peer)
            core[t, k].start()
        fa[t] = rdma(lg.at[t, 1 - x, 1 - y, :, lo], r1a.at[t, 0], fas.at[t], far.at[t], x_peer)
        fb[t] = rdma(lg.at[t, 1 - x, 1 - y, :, hi], r1b.at[t, 0], fbs.at[t], fbr.at[t], y_peer)
        ga[t] = rdma(lg.at[t, 1 - x, y, :, lo], r1a.at[t, 1], gas.at[t], gar.at[t], x_peer)
        gb[t] = rdma(lg.at[t, x, 1 - y, :, hi], r1b.at[t, 1], gbs.at[t], gbr.at[t], y_peer)
        ha[t] = rdma(lg.at[t, x, 1 - y, :, lo], r2a.at[t], has.at[t], har.at[t], y_peer)
        hb[t] = rdma(lg.at[t, 1 - x, y, :, hi], r2b.at[t], hbs.at[t], hbr.at[t], x_peer)
        if t:
            zc[t] = rdma(lg.at[t, x, y], rz.at[t], zs.at[t], zr.at[t], (gx, zof(t), y))

    def add(*terms):
        total = terms[0].astype(f32)
        for term in terms[1:]:
            total = total + term.astype(f32)
        return total

    def over_rows(step):
        @pl.loop(0, tiles)
        def _(i):
            step(pl.ds(pl.multiple_of(i * TILE, TILE), TILE))

    def stage_core(t):
        loads[t].wait()
        for k, (bx, by) in enumerate(blocks):
            core[t, k].wait_recv()

            def step(r):
                lg[t, bx, by, r, :] = add(lg[t, bx, by, r, :], cr[t, k, r, :]).astype(jnp.bfloat16)
            over_rows(step)
            if k == 0:
                fa[t].start()
                fb[t].start()
            elif k == 1:
                ga[t].start()
            elif k == 2:
                gb[t].start()

    def stage_first(t):
        fa[t].wait_recv()
        fb[t].wait_recv()

        def step(r):
            lg[t, x, 1 - y, r, lo] = add(lg[t, x, 1 - y, r, lo], r1a[t, 0, r, :]).astype(jnp.bfloat16)
            lg[t, 1 - x, y, r, hi] = add(lg[t, 1 - x, y, r, hi], r1b[t, 0, r, :]).astype(jnp.bfloat16)
        over_rows(step)
        ha[t].start()
        hb[t].start()

    def stage_second(t):
        for copy in (ga[t], gb[t], ha[t], hb[t]):
            copy.wait_recv()
        if t == 0:
            return

        def step(r):
            lg[t, x, y, r, lo] = add(lg[t, x, y, r, lo], r1a[t, 1, r, :], r2a[t, r, :]).astype(jnp.bfloat16)
            lg[t, x, y, r, hi] = add(lg[t, x, y, r, hi], r1b[t, 1, r, :], r2b[t, r, :]).astype(jnp.bfloat16)
        over_rows(step)
        zc[t].start()

    stage_core(rs_order[0])
    for i, t in enumerate(rs_order):
        stage_first(t)
        if i + 1 < nz:
            stage_core(rs_order[i + 1])
        stage_second(t)
    for t in rs_order:
        if t:
            zc[t].wait_recv()
    for copy in small:
        copy.wait()

    def final(i, carry):
        r = pl.ds(pl.multiple_of(i * TILE, TILE), TILE)
        left = add(lg[0, x, y, r, lo], r1a[0, 1, r, :], r2a[0, r, :], *[rz[t, r, lo] for t in range(1, nz)])
        right = add(lg[0, x, y, r, hi], r1b[0, 1, r, :], r2b[0, r, :], *[rz[t, r, hi] for t in range(1, nz)])
        summed[r, lo] = left
        summed[r, hi] = right
        left, right = left * left, right * right
        own[r, :] = jnp.sum(left, axis=1, keepdims=True) + jnp.sum(right, axis=1, keepdims=True)
        return (carry[0] + left, carry[1] + right)

    zero = jnp.zeros((TILE, half), f32)
    left, right = lax.fori_loop(0, tiles, final, (zero, zero))
    st[0:1, lo] = jnp.sum(left, axis=0, keepdims=True)
    st[0:1, hi] = jnp.sum(right, axis=0, keepdims=True)
    st[1:2, :] = jnp.broadcast_to(jnp.sum(row_state[...], axis=1, keepdims=True), (1, columns))

    me = gx * 2 + y
    sends = []
    for k, peer in enumerate(plane):
        sends.append(rdma(st, st1.at[me], s1s.at[k], s1r.at[k], peer))
        sends[-1].start()
    st1[me] = st[...]
    for t in rs_order:
        for k in range(len(blocks)):
            core[t, k].wait_send()
        for copy in (fa[t], fb[t], ga[t], gb[t], ha[t], hb[t]):
            copy.wait_send()
        if t:
            zc[t].wait_send()
    for copy in sends:
        copy.wait_recv()
    total = st1[0]
    for k in range(1, nx * 2):
        total = total + st1[k]
    tot[...] = total
    line_sends = []
    for t in range(1, nz):
        line_sends.append(rdma(tot, st2.at[z], s2s.at[t], s2r.at[t], (gx, zof(t), y)))
        line_sends[-1].start()
    st2[z] = total
    diagonal = lax.broadcasted_iota(jnp.int32, (rows, rows), 0) == lax.broadcasted_iota(jnp.int32, (rows, rows), 1)
    state_down = jnp.sum(jnp.where(diagonal, jnp.broadcast_to(row_state[...], (rows, rows)), 0.0), axis=1, keepdims=True)
    for copy in line_sends:
        copy.wait_recv()
    total = st2[0]
    for k in range(1, nz):
        total = total + st2[k]
    column_sum = total[0:1, :]
    norm_square = jnp.sum(column_sum, axis=1, keepdims=True)
    state_sum = total[1:2, 0:1]
    clip_level = 0.5 * math.sqrt(full_width * columns)
    factor = jnp.minimum(jnp.float32(1.0), clip_level / jnp.sqrt(norm_square + 1e-06))
    square_factor = factor * factor
    column_next = beta_two * col_state[...] + (1.0 - beta_two) * (square_factor * column_sum / full_width)
    row_average = (beta_two * state_sum + (1.0 - beta_two) * (square_factor * norm_square / columns)) / full_width
    row_next = beta_two * state_down + (1.0 - beta_two) * (square_factor * own[...] / columns)
    own[...] = (step_size * factor) / jnp.sqrt(row_next / row_average)
    col_scale = 1.0 / jnp.sqrt(column_next)

    def update(r):
        new = params[r, :].astype(f32) - (summed[r, :] * own[r, :]) * col_scale
        full[x, c, z, y, r, :] = new.astype(jnp.bfloat16)
    over_rows(update)

    def same(view, ssem, rsem, peer):
        return rdma(view, view, ssem, rsem, peer)

    gz, q1a, q1b, q2a, q2b, q3a, q3b, gc = {}, {}, {}, {}, {}, {}, {}, {}
    for t in range(nz):
        u = zof(t)
        if t:
            gz[t] = rdma(full.at[x, c, z, y], full.at[x, c, z, y], gzs.at[t], gzr.at[t], (gx, u, y))
        q1a[t] = same(full.at[x, c, u, y, :, lo], q1as.at[t], q1ar.at[t], y_peer)
        q1b[t] = same(full.at[x, c, u, y, :, hi], q1bs.at[t], q1br.at[t], x_peer)
        q2a[t] = same(full.at[x, c, u, y, :, lo], q2as.at[t], q2ar.at[t], x_peer)
        q2b[t] = same(full.at[x, c, u, y, :, hi], q2bs.at[t], q2br.at[t], y_peer)
        q3a[t] = same(full.at[x, c, u, 1 - y, :, lo], q3as.at[t], q3ar.at[t], x_peer)
        q3b[t] = same(full.at[1 - x, c, u, y, :, hi], q3bs.at[t], q3br.at[t], y_peer)
        for k, (bx, by) in enumerate(blocks):
            gc[t, k] = same(full.at[bx, c, u, by], gcs.at[t, k], gcr.at[t, k], core_peer)

    def gather_own(t):
        if t:
            gz[t].wait_recv()
        for copy in (q1a[t], q1b[t], q2a[t], q2b[t]):
            copy.start()
        gc[t, 3].start()

    def gather_cross(t):
        q1a[t].wait_recv()
        q1b[t].wait_recv()
        q3a[t].start()
        q3b[t].start()

    def gather_side(t):
        q2a[t].wait_recv()
        gc[t, 1].start()
        q2b[t].wait_recv()
        gc[t, 2].start()

    def gather_far(t):
        q3a[t].wait_recv()
        q3b[t].wait_recv()
        gc[t, 0].start()

    q1a[0].start()
    q1b[0].start()
    for t in range(1, nz):
        gz[t].start()
    q2a[0].start()
    q2b[0].start()
    gc[0, 3].start()
    new_ref[...] = full[x, c, z, y]
    col_ref[...] = column_next
    row_ref[...] = jnp.sum(jnp.where(diagonal, jnp.broadcast_to(row_next, (rows, rows)), 0.0), axis=0, keepdims=True)
    gather_cross(0)
    for t in range(1, nz):
        gather_own(t)
        gather_side(t - 1)
        gather_far(t - 1)
        gather_cross(t)
    gather_side(nz - 1)
    gather_far(nz - 1)
    for copy in sends + line_sends:
        copy.wait_send()
    for t in range(nz):
        if t:
            gz[t].wait_send()
        for copy in (q1a[t], q1b[t], q2a[t], q2b[t], q3a[t], q3b[t]):
            copy.wait_send()
        for k in range(len(blocks)):
            gc[t, k].wait_send()
            gc[t, k].wait_recv()


def write_out(*refs):
    count = (len(refs) - 1) // 2
    sem = refs[-1]
    copies = [pltpu.make_async_copy(refs[k], refs[count + k], sem.at[k]) for k in range(count)]
    for copy in copies:
        copy.start()
    for copy in copies:
        copy.wait()


def fused(nx, nz, grad_bucket, parameters, row_state, column_state):
    _, _, full_width, columns = grad_bucket.shape
    rows = parameters.shape[1]
    half = columns // 2
    bf16, f32 = jnp.bfloat16, jnp.float32
    vmem = pl.BlockSpec(memory_space=pltpu.VMEM)
    hbm = pl.BlockSpec(memory_space=pltpu.HBM)
    dma = pltpu.SemaphoreType.DMA
    shapes = [((rows, columns), bf16), ((1, rows), f32), ((1, columns), f32), ((2, 2, nz, 2, rows, columns), bf16)]
    held = 2 * columns * (rows + full_width) + 4 * (columns + -(-rows // 128) * 128)
    results = pl.pallas_call(
        functools.partial(kernel, nx, nz),
        out_shape=tuple(pltpu.VMEM(*shape) for shape in shapes),
        in_specs=[hbm] * 4,
        out_specs=(vmem,) * 4,
        scratch_shapes=[
            pltpu.VMEM((nz, 2, 2, rows, columns), bf16),
            pltpu.VMEM((nz, 4, rows, columns), bf16),
            pltpu.VMEM((nz, 2, rows, half), bf16),
            pltpu.VMEM((nz, 2, rows, half), bf16),
            pltpu.VMEM((nz, rows, half), bf16),
            pltpu.VMEM((nz, rows, half), bf16),
            pltpu.VMEM((nz, rows, columns), bf16),
            pltpu.VMEM((rows, columns), f32),
            pltpu.VMEM((rows, 1), f32),
            pltpu.VMEM((2, columns), f32),
            pltpu.VMEM((nx * 2, 2, columns), f32),
            pltpu.VMEM((2, columns), f32),
            pltpu.VMEM((nz, 2, columns), f32),
            pltpu.VMEM((rows, columns), bf16),
            pltpu.VMEM((1, rows), f32),
            pltpu.VMEM((1, columns), f32),
        ] + [dma((nz,)), dma((3,))] + [dma((nz, 4))] * 2 + [dma((nz,))] * 14
        + [dma((nx * 2,))] * 2 + [dma((nz,))] * 16 + [dma((nz, 4))] * 2,
        compiler_params=pltpu.CompilerParams(
            collective_id=0, has_side_effects=True, vmem_limit_bytes=VMEM_BYTES - held),
    )(grad_bucket.reshape(2, 2, nz, 2, rows, columns), parameters[0], row_state, column_state)
    new, row, col, full = pl.pallas_call(
        write_out,
        out_shape=tuple(jax.ShapeDtypeStruct(*shape) for shape in shapes),
        in_specs=[vmem] * 4,
        out_specs=(hbm,) * 4,
        scratch_shapes=[dma((4,))],
        compiler_params=pltpu.CompilerParams(vmem_limit_bytes=4 * 1024 * 1024),
    )(*[pltpu.with_memory_space_constraint(result, pltpu.VMEM) for result in results])
    return (new[None], row, col, full.reshape(full_width, columns))


def solution(mesh):
    nx, nz, ny = (mesh.shape[a] for a in AXES)
    in_specs = (
        P(AXES, None, None, None),
        P(None, AXES, None),
        P(None, AXES),
        P(),
    )
    out_specs = (P(None, AXES, None), P(None, AXES), P(), P())
    fits = nx == 4 and ny == 2 and nz & (nz - 1) == 0

    def body(grad_bucket, parameters, row_state, column_state):
        if fits and grad_bucket.shape[1] == 1 and parameters.shape[1] % TILE == 0:
            return fused(nx, nz, grad_bucket, parameters, row_state, column_state)
        return shards(grad_bucket, parameters, row_state, column_state)

    return jax.shard_map(body, mesh=mesh, in_specs=in_specs, out_specs=out_specs, check_vma=False)
```

```python
import functools
import math

import jax
import jax.numpy as jnp
from jax import lax
from jax.experimental import pallas as pl
from jax.experimental.pallas import tpu as pltpu
from jax.sharding import PartitionSpec as P

beta_two = 0.8
step_size = 0.5
AXES = ("gx", "gy", "gz")
TILE = 16
VMEM_BYTES = 67043328 - 131072


def shards(grad_bucket, parameters, row_state, column_state):
    local_grad = grad_bucket[0].astype(jnp.float32)
    layer_count, full_width, columns = local_grad.shape
    summed = lax.psum_scatter(local_grad, AXES, scatter_dimension=1, tiled=True)
    clip_level = 0.5 * math.sqrt(layer_count * full_width * columns)
    squares = summed * summed
    norm_square = lax.psum(jnp.sum(squares), AXES)
    factor = jnp.minimum(jnp.float32(1.0), clip_level / jnp.sqrt(norm_square + 1e-06))
    clipped = factor * summed
    clipped_square = clipped * clipped
    row_next = beta_two * row_state + (1.0 - beta_two) * jnp.mean(clipped_square, axis=2)
    column_part, row_total = lax.psum((jnp.sum(clipped_square, axis=1), jnp.sum(row_next, axis=1)), AXES)
    column_next = beta_two * column_state + (1.0 - beta_two) * column_part / full_width
    row_average = row_total / full_width
    second = row_next[:, :, None] * column_next[:, None, :] / row_average[:, None, None]
    update = clipped / jnp.sqrt(second)
    new_parameters = (parameters.astype(jnp.float32) - step_size * update).astype(jnp.bfloat16)
    first_layer = lax.all_gather(new_parameters[0], AXES, axis=0, tiled=True)
    return (new_parameters, row_next, column_next, first_layer)


def flip(index, mask, size):
    out, bit = 0, 1
    while bit < size:
        out = out + bit * (((index // bit) % 2 + (mask // bit) % 2) % 2)
        bit *= 2
    return out


def kernel(nx, nz, grad, params_in, row_in, col_in, new_ref, row_ref, col_ref, full,
           lg, cr, r1a, r1b, r2a, r2b, rz, summed, own, st, st1, tot, st2, params, row_state, col_state,
           lsem, isem, cs, crv, fas, far, fbs, fbr, gas, gar, gbs, gbr, has, har, hbs, hbr, zs, zr,
           s1s, s1r, s2s, s2r, gzs, gzr, q1as, q1ar, q1bs, q1br, q2as, q2ar, q2bs, q2br,
           q3as, q3ar, q3bs, q3br, gcs, gcr):
    gx, z, y = lax.axis_index("gx"), lax.axis_index("gy"), lax.axis_index("gz")
    x, c = gx // 2, gx % 2
    rows, columns = params.shape
    half = columns // 2
    full_width = rows * 4 * nz * 2
    core_peer = (x * 2 + 1 - c, z, y)
    x_peer = ((1 - x) * 2 + c, z, y)
    y_peer = (gx, z, 1 - y)
    lo, hi = pl.ds(0, half), pl.ds(half, half)
    tiles = rows // TILE
    f32 = jnp.float32
    blocks = [(1 - x, 1 - y), (1 - x, y), (x, 1 - y), (x, y)]

    def zof(t):
        return flip(z, t, nz)

    def rdma(src, dst, ssem, rsem, peer):
        return pltpu.make_async_remote_copy(
            src_ref=src, dst_ref=dst, send_sem=ssem, recv_sem=rsem,
            device_id=peer, device_id_type=pl.DeviceIdType.MESH)

    rs_order = [2, 3, 1, 0] if nz == 4 else list(range(nz - 1, -1, -1))
    loads = {t: pltpu.make_async_copy(grad.at[:, c, zof(t)], lg.at[t], lsem.at[t]) for t in rs_order}
    for t in rs_order:
        loads[t].start()
    small = [pltpu.make_async_copy(src, dst, isem.at[k]) for k, (src, dst) in enumerate(
        [(params_in, params), (row_in, row_state), (col_in, col_state)])]
    for copy in small:
        copy.start()

    barrier = pltpu.get_barrier_semaphore()
    plane = [((gx + a) % nx, z, (y + b) % 2) for a in range(nx) for b in range(2) if (a, b) != (0, 0)]
    line = [(gx, zof(t), y) for t in range(1, nz)]
    for peer in line + plane:
        pl.semaphore_signal(barrier, inc=1, device_id=peer, device_id_type=pl.DeviceIdType.MESH)
    pl.semaphore_wait(barrier, len(plane) + len(line))

    core, fa, fb, ga, gb, ha, hb, zc = {}, {}, {}, {}, {}, {}, {}, {}
    for t in rs_order:
        for k, (bx, by) in enumerate(blocks):
            core[t, k] = rdma(grad.at[bx, 1 - c, zof(t), by], cr.at[t, k], cs.at[t, k], crv.at[t, k], core_peer)
            core[t, k].start()
        fa[t] = rdma(lg.at[t, 1 - x, 1 - y, :, lo], r1a.at[t, 0], fas.at[t], far.at[t], x_peer)
        fb[t] = rdma(lg.at[t, 1 - x, 1 - y, :, hi], r1b.at[t, 0], fbs.at[t], fbr.at[t], y_peer)
        ga[t] = rdma(lg.at[t, 1 - x, y, :, lo], r1a.at[t, 1], gas.at[t], gar.at[t], x_peer)
        gb[t] = rdma(lg.at[t, x, 1 - y, :, hi], r1b.at[t, 1], gbs.at[t], gbr.at[t], y_peer)
        ha[t] = rdma(lg.at[t, x, 1 - y, :, lo], r2a.at[t], has.at[t], har.at[t], y_peer)
        hb[t] = rdma(lg.at[t, 1 - x, y, :, hi], r2b.at[t], hbs.at[t], hbr.at[t], x_peer)
        if t:
            zc[t] = rdma(lg.at[t, x, y], rz.at[t], zs.at[t], zr.at[t], (gx, zof(t), y))

    def add(*terms):
        total = terms[0].astype(f32)
        for term in terms[1:]:
            total = total + term.astype(f32)
        return total

    def over_rows(step):
        @pl.loop(0, tiles)
        def _(i):
            step(pl.ds(pl.multiple_of(i * TILE, TILE), TILE))

    def stage_core(t):
        loads[t].wait()
        for k, (bx, by) in enumerate(blocks):
            core[t, k].wait_recv()

            def step(r):
                lg[t, bx, by, r, :] = add(lg[t, bx, by, r, :], cr[t, k, r, :]).astype(jnp.bfloat16)
            over_rows(step)
            if k == 0:
                fa[t].start()
                fb[t].start()
            elif k == 1:
                ga[t].start()
            elif k == 2:
                gb[t].start()

    def stage_first(t):
        fa[t].wait_recv()
        fb[t].wait_recv()

        def step(r):
            lg[t, x, 1 - y, r, lo] = add(lg[t, x, 1 - y, r, lo], r1a[t, 0, r, :]).astype(jnp.bfloat16)
            lg[t, 1 - x, y, r, hi] = add(lg[t, 1 - x, y, r, hi], r1b[t, 0, r, :]).astype(jnp.bfloat16)
        over_rows(step)
        ha[t].start()
        hb[t].start()

    def stage_second(t):
        for copy in (ga[t], gb[t], ha[t], hb[t]):
            copy.wait_recv()
        if t == 0:
            return

        def step(r):
            lg[t, x, y, r, lo] = add(lg[t, x, y, r, lo], r1a[t, 1, r, :], r2a[t, r, :]).astype(jnp.bfloat16)
            lg[t, x, y, r, hi] = add(lg[t, x, y, r, hi], r1b[t, 1, r, :], r2b[t, r, :]).astype(jnp.bfloat16)
        over_rows(step)
        zc[t].start()

    stage_core(rs_order[0])
    for i, t in enumerate(rs_order):
        stage_first(t)
        if i + 1 < nz:
            stage_core(rs_order[i + 1])
        else:
            for copy in small:
                copy.wait()
            st[1:2, :] = jnp.broadcast_to(jnp.sum(row_state[...], axis=1, keepdims=True), (1, columns))
            early = [k for k in rs_order[:-2] if k]
            for k in early:
                zc[k].wait_recv()

            def gathered(r):
                summed[r, :] = add(lg[0, x, y, r, :], *[rz[k, r, :] for k in early])
            over_rows(gathered)
        stage_second(t)
    for t in rs_order[-2:]:
        if t:
            zc[t].wait_recv()
    late = [t for t in rs_order[-2:] if t]

    def final(i, carry):
        r = pl.ds(pl.multiple_of(i * TILE, TILE), TILE)
        left = add(summed[r, lo], r1a[0, 1, r, :], r2a[0, r, :], *[rz[t, r, lo] for t in late])
        right = add(summed[r, hi], r1b[0, 1, r, :], r2b[0, r, :], *[rz[t, r, hi] for t in late])
        summed[r, lo] = left
        summed[r, hi] = right
        left, right = left * left, right * right
        own[r, :] = jnp.sum(left, axis=1, keepdims=True) + jnp.sum(right, axis=1, keepdims=True)
        return (carry[0] + left, carry[1] + right)

    zero = jnp.zeros((TILE, half), f32)
    left, right = lax.fori_loop(0, tiles, final, (zero, zero))
    st[0:1, lo] = jnp.sum(left, axis=0, keepdims=True)
    st[0:1, hi] = jnp.sum(right, axis=0, keepdims=True)

    me = gx * 2 + y
    sends = []
    for k, peer in enumerate(plane):
        sends.append(rdma(st, st1.at[me], s1s.at[k], s1r.at[k], peer))
        sends[-1].start()
    st1[me] = st[...]
    for t in rs_order:
        for k in range(len(blocks)):
            core[t, k].wait_send()
        for copy in (fa[t], fb[t], ga[t], gb[t], ha[t], hb[t]):
            copy.wait_send()
        if t:
            zc[t].wait_send()
    for copy in sends:
        copy.wait_recv()
    total = st1[0]
    for k in range(1, nx * 2):
        total = total + st1[k]
    tot[...] = total
    line_sends = []
    for t in range(1, nz):
        line_sends.append(rdma(tot, st2.at[z], s2s.at[t], s2r.at[t], (gx, zof(t), y)))
        line_sends[-1].start()
    st2[z] = total
    diagonal = lax.broadcasted_iota(jnp.int32, (rows, rows), 0) == lax.broadcasted_iota(jnp.int32, (rows, rows), 1)
    state_down = jnp.sum(jnp.where(diagonal, jnp.broadcast_to(row_state[...], (rows, rows)), 0.0), axis=1, keepdims=True)
    for copy in line_sends:
        copy.wait_recv()
    total = st2[0]
    for k in range(1, nz):
        total = total + st2[k]
    column_sum = total[0:1, :]
    norm_square = jnp.sum(column_sum, axis=1, keepdims=True)
    state_sum = total[1:2, 0:1]
    clip_level = 0.5 * math.sqrt(full_width * columns)
    factor = jnp.minimum(jnp.float32(1.0), clip_level / jnp.sqrt(norm_square + 1e-06))
    square_factor = factor * factor
    column_next = beta_two * col_state[...] + (1.0 - beta_two) * (square_factor * column_sum / full_width)
    row_average = (beta_two * state_sum + (1.0 - beta_two) * (square_factor * norm_square / columns)) / full_width
    row_next = beta_two * state_down + (1.0 - beta_two) * (square_factor * own[...] / columns)
    own[...] = (step_size * factor) / jnp.sqrt(row_next / row_average)
    col_scale = 1.0 / jnp.sqrt(column_next)

    def update(r):
        new = params[r, :].astype(f32) - (summed[r, :] * own[r, :]) * col_scale
        full[x, c, z, y, r, :] = new.astype(jnp.bfloat16)
    over_rows(update)

    def same(view, ssem, rsem, peer):
        return rdma(view, view, ssem, rsem, peer)

    gz, q1a, q1b, q2a, q2b, q3a, q3b, gc = {}, {}, {}, {}, {}, {}, {}, {}
    for t in range(nz):
        u = zof(t)
        if t:
            gz[t] = rdma(full.at[x, c, z, y], full.at[x, c, z, y], gzs.at[t], gzr.at[t], (gx, u, y))
        q1a[t] = same(full.at[x, c, u, y, :, lo], q1as.at[t], q1ar.at[t], y_peer)
        q1b[t] = same(full.at[x, c, u, y, :, hi], q1bs.at[t], q1br.at[t], x_peer)
        q2a[t] = same(full.at[x, c, u, y, :, lo], q2as.at[t], q2ar.at[t], x_peer)
        q2b[t] = same(full.at[x, c, u, y, :, hi], q2bs.at[t], q2br.at[t], y_peer)
        q3a[t] = same(full.at[x, c, u, 1 - y, :, lo], q3as.at[t], q3ar.at[t], x_peer)
        q3b[t] = same(full.at[1 - x, c, u, y, :, hi], q3bs.at[t], q3br.at[t], y_peer)
        for k, (bx, by) in enumerate(blocks):
            gc[t, k] = same(full.at[bx, c, u, by], gcs.at[t, k], gcr.at[t, k], core_peer)

    def gather_own(t):
        if t:
            gz[t].wait_recv()
        for copy in (q1a[t], q1b[t], q2a[t], q2b[t]):
            copy.start()
        gc[t, 3].start()

    def gather_cross(t):
        q1a[t].wait_recv()
        q1b[t].wait_recv()
        q3a[t].start()
        q3b[t].start()

    def gather_side(t):
        q2a[t].wait_recv()
        gc[t, 1].start()
        q2b[t].wait_recv()
        gc[t, 2].start()

    def gather_far(t):
        q3a[t].wait_recv()
        q3b[t].wait_recv()
        gc[t, 0].start()

    q1a[0].start()
    q1b[0].start()
    for t in range(1, nz):
        gz[t].start()
    q2a[0].start()
    q2b[0].start()
    gc[0, 3].start()
    new_ref[...] = full[x, c, z, y]
    col_ref[...] = column_next
    row_ref[...] = jnp.sum(jnp.where(diagonal, jnp.broadcast_to(row_next, (rows, rows)), 0.0), axis=0, keepdims=True)
    gather_cross(0)
    for t in range(1, nz):
        gather_own(t)
        gather_side(t - 1)
        gather_far(t - 1)
        gather_cross(t)
    gather_side(nz - 1)
    gather_far(nz - 1)
    for copy in sends + line_sends:
        copy.wait_send()
    for t in range(nz):
        if t:
            gz[t].wait_send()
        for copy in (q1a[t], q1b[t], q2a[t], q2b[t], q3a[t], q3b[t]):
            copy.wait_send()
        for k in range(len(blocks)):
            gc[t, k].wait_send()
            gc[t, k].wait_recv()


def write_out(nz, new, row, col, full, new_out, row_out, col_out, full_out, sem):
    pairs = [(full.at[a, b, u], full_out.at[a, b, u]) for a in range(2) for b in range(2) for u in range(nz)]
    pairs += [(new, new_out), (row, row_out), (col, col_out)]
    copies = [pltpu.make_async_copy(src, dst, sem.at[k]) for k, (src, dst) in enumerate(pairs)]
    for copy in copies:
        copy.start()
    for copy in copies:
        copy.wait()


def fused(nx, nz, grad_bucket, parameters, row_state, column_state):
    _, _, full_width, columns = grad_bucket.shape
    rows = parameters.shape[1]
    half = columns // 2
    bf16, f32 = jnp.bfloat16, jnp.float32
    vmem = pl.BlockSpec(memory_space=pltpu.VMEM)
    hbm = pl.BlockSpec(memory_space=pltpu.HBM)
    dma = pltpu.SemaphoreType.DMA
    shapes = [((rows, columns), bf16), ((1, rows), f32), ((1, columns), f32), ((2, 2, nz, 2, rows, columns), bf16)]
    held = 2 * columns * (rows + full_width) + 4 * (columns + -(-rows // 128) * 128)
    results = pl.pallas_call(
        functools.partial(kernel, nx, nz),
        out_shape=tuple(pltpu.VMEM(*shape) for shape in shapes),
        in_specs=[hbm] * 4,
        out_specs=(vmem,) * 4,
        scratch_shapes=[
            pltpu.VMEM((nz, 2, 2, rows, columns), bf16),
            pltpu.VMEM((nz, 4, rows, columns), bf16),
            pltpu.VMEM((nz, 2, rows, half), bf16),
            pltpu.VMEM((nz, 2, rows, half), bf16),
            pltpu.VMEM((nz, rows, half), bf16),
            pltpu.VMEM((nz, rows, half), bf16),
            pltpu.VMEM((nz, rows, columns), bf16),
            pltpu.VMEM((rows, columns), f32),
            pltpu.VMEM((rows, 1), f32),
            pltpu.VMEM((2, columns), f32),
            pltpu.VMEM((nx * 2, 2, columns), f32),
            pltpu.VMEM((2, columns), f32),
            pltpu.VMEM((nz, 2, columns), f32),
            pltpu.VMEM((rows, columns), bf16),
            pltpu.VMEM((1, rows), f32),
            pltpu.VMEM((1, columns), f32),
        ] + [dma((nz,)), dma((3,))] + [dma((nz, 4))] * 2 + [dma((nz,))] * 14
        + [dma((nx * 2,))] * 2 + [dma((nz,))] * 16 + [dma((nz, 4))] * 2,
        compiler_params=pltpu.CompilerParams(
            collective_id=0, has_side_effects=True, vmem_limit_bytes=VMEM_BYTES - held),
    )(grad_bucket.reshape(2, 2, nz, 2, rows, columns), parameters[0], row_state, column_state)
    new, row, col, full = pl.pallas_call(
        functools.partial(write_out, nz),
        out_shape=tuple(jax.ShapeDtypeStruct(*shape) for shape in shapes),
        in_specs=[vmem] * 4,
        out_specs=(hbm,) * 4,
        scratch_shapes=[dma((4 * nz + 3,))],
        compiler_params=pltpu.CompilerParams(vmem_limit_bytes=4 * 1024 * 1024),
    )(*[pltpu.with_memory_space_constraint(result, pltpu.VMEM) for result in results])
    return (new[None], row, col, full.reshape(full_width, columns))


def solution(mesh):
    nx, nz, ny = (mesh.shape[a] for a in AXES)
    in_specs = (
        P(AXES, None, None, None),
        P(None, AXES, None),
        P(None, AXES),
        P(),
    )
    out_specs = (P(None, AXES, None), P(None, AXES), P(), P())
    fits = nx == 4 and ny == 2 and nz & (nz - 1) == 0

    def body(grad_bucket, parameters, row_state, column_state):
        if fits and grad_bucket.shape[1] == 1 and parameters.shape[1] % TILE == 0:
            return fused(nx, nz, grad_bucket, parameters, row_state, column_state)
        return shards(grad_bucket, parameters, row_state, column_state)

    return jax.shard_map(body, mesh=mesh, in_specs=in_specs, out_specs=out_specs, check_vma=False)
```

```python
import functools
import math

import jax
import jax.numpy as jnp
from jax import lax
from jax.experimental import pallas as pl
from jax.experimental.pallas import tpu as pltpu
from jax.sharding import PartitionSpec as P

beta_two = 0.8
step_size = 0.5
AXES = ("gx", "gy", "gz")
TILE = 16
VMEM_BYTES = 67043328 - 131072


def shards(grad_bucket, parameters, row_state, column_state):
    local_grad = grad_bucket[0].astype(jnp.float32)
    layer_count, full_width, columns = local_grad.shape
    summed = lax.psum_scatter(local_grad, AXES, scatter_dimension=1, tiled=True)
    clip_level = 0.5 * math.sqrt(layer_count * full_width * columns)
    squares = summed * summed
    norm_square = lax.psum(jnp.sum(squares), AXES)
    factor = jnp.minimum(jnp.float32(1.0), clip_level / jnp.sqrt(norm_square + 1e-06))
    clipped = factor * summed
    clipped_square = clipped * clipped
    row_next = beta_two * row_state + (1.0 - beta_two) * jnp.mean(clipped_square, axis=2)
    column_part, row_total = lax.psum((jnp.sum(clipped_square, axis=1), jnp.sum(row_next, axis=1)), AXES)
    column_next = beta_two * column_state + (1.0 - beta_two) * column_part / full_width
    row_average = row_total / full_width
    second = row_next[:, :, None] * column_next[:, None, :] / row_average[:, None, None]
    update = clipped / jnp.sqrt(second)
    new_parameters = (parameters.astype(jnp.float32) - step_size * update).astype(jnp.bfloat16)
    first_layer = lax.all_gather(new_parameters[0], AXES, axis=0, tiled=True)
    return (new_parameters, row_next, column_next, first_layer)


def flip(index, mask, size):
    out, bit = 0, 1
    while bit < size:
        out = out + bit * (((index // bit) % 2 + (mask // bit) % 2) % 2)
        bit *= 2
    return out


def kernel(nx, nz, grad, params_in, row_in, col_in, new_ref, row_ref, col_ref, full,
           lg, cr, r1a, r1b, r2a, r2b, rz, summed, own, st, st1, tot, st2, params, row_state, col_state,
           lsem, isem, cs, crv, fas, far, fbs, fbr, gas, gar, gbs, gbr, has, har, hbs, hbr, zs, zr,
           s1s, s1r, s2s, s2r, gzs, gzr, q1as, q1ar, q1bs, q1br, q2as, q2ar, q2bs, q2br,
           q3as, q3ar, q3bs, q3br, gcs, gcr):
    gx, z, y = lax.axis_index("gx"), lax.axis_index("gy"), lax.axis_index("gz")
    x, c = gx // 2, gx % 2
    rows, columns = params.shape
    half = columns // 2
    full_width = rows * 4 * nz * 2
    core_peer = (x * 2 + 1 - c, z, y)
    x_peer = ((1 - x) * 2 + c, z, y)
    y_peer = (gx, z, 1 - y)
    lo, hi = pl.ds(0, half), pl.ds(half, half)
    tiles = rows // TILE
    f32 = jnp.float32
    blocks = [(1 - x, 1 - y), (1 - x, y), (x, 1 - y), (x, y)]

    def zof(t):
        return flip(z, t, nz)

    def rdma(src, dst, ssem, rsem, peer):
        return pltpu.make_async_remote_copy(
            src_ref=src, dst_ref=dst, send_sem=ssem, recv_sem=rsem,
            device_id=peer, device_id_type=pl.DeviceIdType.MESH)

    rs_order = [2, 3, 1, 0] if nz == 4 else list(range(nz - 1, -1, -1))
    loads = {t: pltpu.make_async_copy(grad.at[:, c, zof(t)], lg.at[t], lsem.at[t]) for t in rs_order}
    for t in rs_order:
        loads[t].start()
    small = [pltpu.make_async_copy(src, dst, isem.at[k]) for k, (src, dst) in enumerate(
        [(params_in, params), (row_in, row_state), (col_in, col_state)])]
    for copy in small:
        copy.start()

    barrier = pltpu.get_barrier_semaphore()
    plane = [((gx + a) % nx, z, (y + b) % 2) for a in range(nx) for b in range(2) if (a, b) != (0, 0)]
    line = [(gx, zof(t), y) for t in range(1, nz)]
    for peer in line + plane:
        pl.semaphore_signal(barrier, inc=1, device_id=peer, device_id_type=pl.DeviceIdType.MESH)
    pl.semaphore_wait(barrier, len(plane) + len(line))

    core, fa, fb, ga, gb, ha, hb, zc = {}, {}, {}, {}, {}, {}, {}, {}
    for t in rs_order:
        for k, (bx, by) in enumerate(blocks):
            core[t, k] = rdma(grad.at[bx, 1 - c, zof(t), by], cr.at[t, k], cs.at[t, k], crv.at[t, k], core_peer)
            core[t, k].start()
        fa[t] = rdma(lg.at[t, 1 - x, 1 - y, :, lo], r1a.at[t, 0], fas.at[t], far.at[t], x_peer)
        fb[t] = rdma(lg.at[t, 1 - x, 1 - y, :, hi], r1b.at[t, 0], fbs.at[t], fbr.at[t], y_peer)
        ga[t] = rdma(lg.at[t, 1 - x, y, :, lo], r1a.at[t, 1], gas.at[t], gar.at[t], x_peer)
        gb[t] = rdma(lg.at[t, x, 1 - y, :, hi], r1b.at[t, 1], gbs.at[t], gbr.at[t], y_peer)
        ha[t] = rdma(lg.at[t, x, 1 - y, :, lo], r2a.at[t], has.at[t], har.at[t], y_peer)
        hb[t] = rdma(lg.at[t, 1 - x, y, :, hi], r2b.at[t], hbs.at[t], hbr.at[t], x_peer)
        if t:
            zc[t] = rdma(lg.at[t, x, y], rz.at[t], zs.at[t], zr.at[t], (gx, zof(t), y))

    def add(*terms):
        total = terms[0].astype(f32)
        for term in terms[1:]:
            total = total + term.astype(f32)
        return total

    def over_rows(step):
        @pl.loop(0, tiles, unroll=True)
        def _(i):
            step(pl.ds(pl.multiple_of(i * TILE, TILE), TILE))

    def stage_core(t):
        loads[t].wait()
        for k, (bx, by) in enumerate(blocks):
            core[t, k].wait_recv()

            def step(r):
                lg[t, bx, by, r, :] = add(lg[t, bx, by, r, :], cr[t, k, r, :]).astype(jnp.bfloat16)
            over_rows(step)
            if k == 0:
                fa[t].start()
                fb[t].start()
            elif k == 1:
                ga[t].start()
            elif k == 2:
                gb[t].start()

    def stage_first(t):
        fa[t].wait_recv()
        fb[t].wait_recv()

        def step(r):
            lg[t, x, 1 - y, r, lo] = add(lg[t, x, 1 - y, r, lo], r1a[t, 0, r, :]).astype(jnp.bfloat16)
            lg[t, 1 - x, y, r, hi] = add(lg[t, 1 - x, y, r, hi], r1b[t, 0, r, :]).astype(jnp.bfloat16)
        over_rows(step)
        ha[t].start()
        hb[t].start()

    def stage_second(t):
        for copy in (ga[t], gb[t], ha[t], hb[t]):
            copy.wait_recv()
        if t == 0:
            return

        def step(r):
            lg[t, x, y, r, lo] = add(lg[t, x, y, r, lo], r1a[t, 1, r, :], r2a[t, r, :]).astype(jnp.bfloat16)
            lg[t, x, y, r, hi] = add(lg[t, x, y, r, hi], r1b[t, 1, r, :], r2b[t, r, :]).astype(jnp.bfloat16)
        over_rows(step)
        zc[t].start()

    stage_core(rs_order[0])
    for i, t in enumerate(rs_order):
        stage_first(t)
        if i + 1 < nz:
            stage_core(rs_order[i + 1])
        else:
            for copy in small:
                copy.wait()
            st[1:2, :] = jnp.broadcast_to(jnp.sum(row_state[...], axis=1, keepdims=True), (1, columns))
            early = [k for k in rs_order[:-2] if k]
            for k in early:
                zc[k].wait_recv()

            def gathered(r):
                summed[r, :] = add(lg[0, x, y, r, :], *[rz[k, r, :] for k in early])
            over_rows(gathered)
        stage_second(t)
    for t in rs_order[-2:]:
        if t:
            zc[t].wait_recv()
    late = [t for t in rs_order[-2:] if t]

    def final(i, carry):
        r = pl.ds(pl.multiple_of(i * TILE, TILE), TILE)
        left = add(summed[r, lo], r1a[0, 1, r, :], r2a[0, r, :], *[rz[t, r, lo] for t in late])
        right = add(summed[r, hi], r1b[0, 1, r, :], r2b[0, r, :], *[rz[t, r, hi] for t in late])
        summed[r, lo] = left
        summed[r, hi] = right
        left, right = left * left, right * right
        own[r, :] = jnp.sum(left, axis=1, keepdims=True) + jnp.sum(right, axis=1, keepdims=True)
        return (carry[0] + left, carry[1] + right)

    zero = jnp.zeros((TILE, half), f32)
    left, right = lax.fori_loop(0, tiles, final, (zero, zero))
    st[0:1, lo] = jnp.sum(left, axis=0, keepdims=True)
    st[0:1, hi] = jnp.sum(right, axis=0, keepdims=True)

    me = gx * 2 + y
    sends = []
    for k, peer in enumerate(plane):
        sends.append(rdma(st, st1.at[me], s1s.at[k], s1r.at[k], peer))
        sends[-1].start()
    st1[me] = st[...]
    for t in rs_order:
        for k in range(len(blocks)):
            core[t, k].wait_send()
        for copy in (fa[t], fb[t], ga[t], gb[t], ha[t], hb[t]):
            copy.wait_send()
        if t:
            zc[t].wait_send()
    for copy in sends:
        copy.wait_recv()
    total = st1[0]
    for k in range(1, nx * 2):
        total = total + st1[k]
    tot[...] = total
    line_sends = []
    for t in range(1, nz):
        line_sends.append(rdma(tot, st2.at[z], s2s.at[t], s2r.at[t], (gx, zof(t), y)))
        line_sends[-1].start()
    st2[z] = total
    diagonal = lax.broadcasted_iota(jnp.int32, (rows, rows), 0) == lax.broadcasted_iota(jnp.int32, (rows, rows), 1)
    state_down = jnp.sum(jnp.where(diagonal, jnp.broadcast_to(row_state[...], (rows, rows)), 0.0), axis=1, keepdims=True)
    for copy in line_sends:
        copy.wait_recv()
    total = st2[0]
    for k in range(1, nz):
        total = total + st2[k]
    column_sum = total[0:1, :]
    norm_square = jnp.sum(column_sum, axis=1, keepdims=True)
    state_sum = total[1:2, 0:1]
    clip_level = 0.5 * math.sqrt(full_width * columns)
    factor = jnp.minimum(jnp.float32(1.0), clip_level / jnp.sqrt(norm_square + 1e-06))
    square_factor = factor * factor
    column_next = beta_two * col_state[...] + (1.0 - beta_two) * (square_factor * column_sum / full_width)
    row_average = (beta_two * state_sum + (1.0 - beta_two) * (square_factor * norm_square / columns)) / full_width
    row_next = beta_two * state_down + (1.0 - beta_two) * (square_factor * own[...] / columns)
    own[...] = (step_size * factor) / jnp.sqrt(row_next / row_average)
    col_scale = 1.0 / jnp.sqrt(column_next)

    def update(r):
        new = params[r, :].astype(f32) - (summed[r, :] * own[r, :]) * col_scale
        full[x, c, z, y, r, :] = new.astype(jnp.bfloat16)
    over_rows(update)

    def same(view, ssem, rsem, peer):
        return rdma(view, view, ssem, rsem, peer)

    gz, q1a, q1b, q2a, q2b, q3a, q3b, gc = {}, {}, {}, {}, {}, {}, {}, {}
    for t in range(nz):
        u = zof(t)
        if t:
            gz[t] = rdma(full.at[x, c, z, y], full.at[x, c, z, y], gzs.at[t], gzr.at[t], (gx, u, y))
        q1a[t] = same(full.at[x, c, u, y, :, lo], q1as.at[t], q1ar.at[t], y_peer)
        q1b[t] = same(full.at[x, c, u, y, :, hi], q1bs.at[t], q1br.at[t], x_peer)
        q2a[t] = same(full.at[x, c, u, y, :, lo], q2as.at[t], q2ar.at[t], x_peer)
        q2b[t] = same(full.at[x, c, u, y, :, hi], q2bs.at[t], q2br.at[t], y_peer)
        q3a[t] = same(full.at[x, c, u, 1 - y, :, lo], q3as.at[t], q3ar.at[t], x_peer)
        q3b[t] = same(full.at[1 - x, c, u, y, :, hi], q3bs.at[t], q3br.at[t], y_peer)
        for k, (bx, by) in enumerate(blocks):
            gc[t, k] = same(full.at[bx, c, u, by], gcs.at[t, k], gcr.at[t, k], core_peer)

    def gather_own(t):
        if t:
            gz[t].wait_recv()
        for copy in (q1a[t], q1b[t], q2a[t], q2b[t]):
            copy.start()
        gc[t, 3].start()

    def gather_cross(t):
        q1a[t].wait_recv()
        q1b[t].wait_recv()
        q3a[t].start()
        q3b[t].start()

    def gather_side(t):
        q2a[t].wait_recv()
        gc[t, 1].start()
        q2b[t].wait_recv()
        gc[t, 2].start()

    def gather_far(t):
        q3a[t].wait_recv()
        q3b[t].wait_recv()
        gc[t, 0].start()

    q1a[0].start()
    q1b[0].start()
    for t in range(1, nz):
        gz[t].start()
    q2a[0].start()
    q2b[0].start()
    gc[0, 3].start()
    new_ref[...] = full[x, c, z, y]
    col_ref[...] = column_next
    row_ref[...] = jnp.sum(jnp.where(diagonal, jnp.broadcast_to(row_next, (rows, rows)), 0.0), axis=0, keepdims=True)
    gather_cross(0)
    for t in range(1, nz):
        gather_own(t)
        gather_side(t - 1)
        gather_far(t - 1)
        gather_cross(t)
    gather_side(nz - 1)
    gather_far(nz - 1)
    for copy in sends + line_sends:
        copy.wait_send()
    for t in range(nz):
        if t:
            gz[t].wait_send()
        for copy in (q1a[t], q1b[t], q2a[t], q2b[t], q3a[t], q3b[t]):
            copy.wait_send()
        for k in range(len(blocks)):
            gc[t, k].wait_send()
            gc[t, k].wait_recv()


def write_out(nz, new, row, col, full, new_out, row_out, col_out, full_out, sem):
    pairs = [(full.at[a, b, u], full_out.at[a, b, u]) for a in range(2) for b in range(2) for u in range(nz)]
    pairs += [(new, new_out), (row, row_out), (col, col_out)]
    copies = [pltpu.make_async_copy(src, dst, sem.at[k]) for k, (src, dst) in enumerate(pairs)]
    for copy in copies:
        copy.start()
    for copy in copies:
        copy.wait()


def fused(nx, nz, grad_bucket, parameters, row_state, column_state):
    _, _, full_width, columns = grad_bucket.shape
    rows = parameters.shape[1]
    half = columns // 2
    bf16, f32 = jnp.bfloat16, jnp.float32
    vmem = pl.BlockSpec(memory_space=pltpu.VMEM)
    hbm = pl.BlockSpec(memory_space=pltpu.HBM)
    dma = pltpu.SemaphoreType.DMA
    shapes = [((rows, columns), bf16), ((1, rows), f32), ((1, columns), f32), ((2, 2, nz, 2, rows, columns), bf16)]
    held = 2 * columns * (rows + full_width) + 4 * (columns + -(-rows // 128) * 128)
    results = pl.pallas_call(
        functools.partial(kernel, nx, nz),
        out_shape=tuple(pltpu.VMEM(*shape) for shape in shapes),
        in_specs=[hbm] * 4,
        out_specs=(vmem,) * 4,
        scratch_shapes=[
            pltpu.VMEM((nz, 2, 2, rows, columns), bf16),
            pltpu.VMEM((nz, 4, rows, columns), bf16),
            pltpu.VMEM((nz, 2, rows, half), bf16),
            pltpu.VMEM((nz, 2, rows, half), bf16),
            pltpu.VMEM((nz, rows, half), bf16),
            pltpu.VMEM((nz, rows, half), bf16),
            pltpu.VMEM((nz, rows, columns), bf16),
            pltpu.VMEM((rows, columns), f32),
            pltpu.VMEM((rows, 1), f32),
            pltpu.VMEM((2, columns), f32),
            pltpu.VMEM((nx * 2, 2, columns), f32),
            pltpu.VMEM((2, columns), f32),
            pltpu.VMEM((nz, 2, columns), f32),
            pltpu.VMEM((rows, columns), bf16),
            pltpu.VMEM((1, rows), f32),
            pltpu.VMEM((1, columns), f32),
        ] + [dma((nz,)), dma((3,))] + [dma((nz, 4))] * 2 + [dma((nz,))] * 14
        + [dma((nx * 2,))] * 2 + [dma((nz,))] * 16 + [dma((nz, 4))] * 2,
        compiler_params=pltpu.CompilerParams(
            collective_id=0, has_side_effects=True, vmem_limit_bytes=VMEM_BYTES - held),
    )(grad_bucket.reshape(2, 2, nz, 2, rows, columns), parameters[0], row_state, column_state)
    new, row, col, full = pl.pallas_call(
        functools.partial(write_out, nz),
        out_shape=tuple(jax.ShapeDtypeStruct(*shape) for shape in shapes),
        in_specs=[vmem] * 4,
        out_specs=(hbm,) * 4,
        scratch_shapes=[dma((4 * nz + 3,))],
        compiler_params=pltpu.CompilerParams(vmem_limit_bytes=4 * 1024 * 1024),
    )(*[pltpu.with_memory_space_constraint(result, pltpu.VMEM) for result in results])
    return (new[None], row, col, full.reshape(full_width, columns))


def solution(mesh):
    nx, nz, ny = (mesh.shape[a] for a in AXES)
    in_specs = (
        P(AXES, None, None, None),
        P(None, AXES, None),
        P(None, AXES),
        P(),
    )
    out_specs = (P(None, AXES, None), P(None, AXES), P(), P())
    fits = nx == 4 and ny == 2 and nz & (nz - 1) == 0

    def body(grad_bucket, parameters, row_state, column_state):
        if fits and grad_bucket.shape[1] == 1 and parameters.shape[1] % TILE == 0:
            return fused(nx, nz, grad_bucket, parameters, row_state, column_state)
        return shards(grad_bucket, parameters, row_state, column_state)

    return jax.shard_map(body, mesh=mesh, in_specs=in_specs, out_specs=out_specs, check_vma=False)
```
